32 devices in a mesh: blk: 8 (over z, y), grp: 4 (over x, core).
Axes of the slice: x: 2, y: 2, z: 4, core: 2. Of those that a mesh axis runs over, the one named last changes fastest.
Arguments:
- embeddings: bfloat16 [4096, 1024], P(('blk', 'grp')), may hold values from -100 to 100
- labels: int32 [4096], P(('blk', 'grp')), may hold values from 0 to 4999, as said below
Outputs:
- anchor_loss: float32 [1024], P(('blk', 'grp'))
- mean_loss: float32 [], replicated
The draws below stay inside these ranges and needn't reach their ends.
Inputs may be any that keep to these rules, and one draw needn't show every extreme that they name: `labels`: A label of 1000 or more belongs to one sample only.
All inputs are finite; a program needn't handle non-finite values.
Results may differ from the reference program's by a relative error of at most 0.0003.
Values may be sent and summed in bfloat16 or wider, within the bound.
A program may use at most 64 MiB of HBM per device.

```python
import math
import jax
import jax.numpy as jnp
from jax import lax

D = 1024
B_DEV = 128
A_DEV = 32
CLASSES = 1000
TOTAL = 4096


def class_labels(key):
    base_key = jax.random.fold_in(key, 11)
    sub_keys = jax.random.split(base_key, 6)
    smallest = jnp.full((TOTAL,), CLASSES - 1, jnp.int32)
    for draw_step in range(4):
        smallest = jnp.minimum(smallest, jax.random.randint(sub_keys[draw_step], (TOTAL,), 0, CLASSES, dtype=jnp.int32))
    class_order = jax.random.permutation(sub_keys[4], jnp.arange(CLASSES, dtype=jnp.int32))
    common_label = class_order[smallest]
    sample_ids = jnp.arange(TOTAL, dtype=jnp.int32)
    common_label = jnp.where(sample_ids == 0, 0, common_label)
    is_anchor = sample_ids % B_DEV < A_DEV
    lone_label = is_anchor & (jax.random.randint(sub_keys[5], (TOTAL,), 0, 16, dtype=jnp.int32) == 0)
    lone_label = lone_label & (sample_ids != 0)
    lone_label = lone_label | (sample_ids == TOTAL - B_DEV + A_DEV - 1)
    return jnp.where(lone_label, CLASSES + sample_ids, common_label).astype(jnp.int32)


def draw_labels(key, part):
    return class_labels(key)


def draw_embeddings(key, part):
    sample_labels = class_labels(key)
    centre_key, noise_key = jax.random.split(jax.random.fold_in(key, 23), 2)
    centroids = jax.random.normal(centre_key, (CLASSES, D), jnp.float32)
    has_class = (sample_labels < CLASSES).astype(jnp.float32)
    class_rows = centroids[jnp.minimum(sample_labels, CLASSES - 1)] * has_class[:, None]
    noise_part = jax.random.normal(noise_key, (TOTAL, D), jnp.float32)
    drawn = 0.8 * class_rows + noise_part
    return jnp.clip(drawn, -100.0, 100.0).astype(jnp.bfloat16)


def setup_inputs(seed: int = 0) -> dict:
    arg_keys = jax.random.split(jax.random.key(seed), 3)
    return {
        "embeddings": draw_embeddings(jax.random.fold_in(arg_keys[2], 71), 0),
        "labels": draw_labels(jax.random.fold_in(arg_keys[2], 71), 0),
    }


def reference(embeddings, labels):
    values = embeddings.astype(jnp.float32)
    unit = (values * lax.rsqrt(lax.optimization_barrier(jnp.sum(values * values, axis=1, keepdims=True)) + 1e-06)).astype(jnp.bfloat16)
    total = unit.shape[0]
    shards = total // B_DEV
    anchor_unit = unit.reshape(shards, B_DEV, unit.shape[1])[:, :A_DEV].reshape(shards * A_DEV, unit.shape[1])
    anchor_lab = labels.reshape(shards, B_DEV)[:, :A_DEV].reshape(shards * A_DEV)
    shard_ids = jnp.arange(shards, dtype=jnp.int32)[:, None] * B_DEV
    anchor_pos = (shard_ids + jnp.arange(A_DEV, dtype=jnp.int32)[None, :]).reshape(shards * A_DEV)
    anchors_all = shards * A_DEV
    width = math.gcd(anchors_all, 512)
    blocks = anchors_all // width
    key_ids = jnp.arange(total, dtype=jnp.int32)

    def one_block(index):
        start = (index * width).astype(jnp.int32)
        anchors = lax.dynamic_slice_in_dim(anchor_unit, start, width, 0)
        anchor_labels = lax.dynamic_slice_in_dim(anchor_lab, start, width, 0)
        anchor_ids = lax.dynamic_slice_in_dim(anchor_pos, start, width, 0)
        score = lax.dot_general(anchors, unit, (((1,), (1,)), ((), ())), preferred_element_type=jnp.float32) * 10.0
        self_mask = anchor_ids[:, None] == key_ids[None, :]
        denom = lax.optimization_barrier(jnp.sum(jnp.where(self_mask, 0.0, jnp.exp(score - 10.0)), axis=1))
        positive = (anchor_labels[:, None] == labels[None, :]) & jnp.logical_not(self_mask)
        pos_sum = lax.optimization_barrier(jnp.sum(jnp.where(positive, score, 0.0), axis=1))
        count = lax.optimization_barrier(jnp.sum(positive.astype(jnp.float32), axis=1))
        return (denom, pos_sum, count)
    denom, pos_sum, count = lax.map(one_block, jnp.arange(blocks, dtype=jnp.int32))
    denom = denom.reshape(anchors_all)
    pos_sum = pos_sum.reshape(anchors_all)
    count = count.reshape(anchors_all)
    valid = count > 0.0
    anchor_loss = jnp.where(valid, jnp.log(denom) + 10.0 - pos_sum / jnp.maximum(count, 1.0), 0.0)
    mean_loss = jnp.sum(anchor_loss) / jnp.maximum(jnp.sum(valid.astype(jnp.float32)), 1.0)
    return (anchor_loss, mean_loss)
```

```python
import functools

import jax
import jax.numpy as jnp
from jax import lax
from jax.experimental import pallas as pl
from jax.experimental.pallas import tpu as pltpu
from jax.sharding import PartitionSpec as P

A_DEV = 32
LANES = 128
MESH = pl.DeviceIdType.MESH


def flip(value, bits):
    out, bit = value, 1
    while bit <= bits:
        if bits & bit:
            out = out + bit - 2 * bit * ((value // bit) % 2)
        bit *= 2
    return out


def partner(value, step, count):
    if count & (count - 1) == 0:
        other = flip(value, step)
        return other, other
    return (value + step) % count, (value + count - step) % count


def kernel(
    sizes, emb_hbm, lab_ref, out_ref,
    emb, keys, anc, lab_k, lab_a, part,
    emb_sem, key_send, key_recv, anc_send, anc_recv, lab_send, lab_k_recv, lab_a_recv, part_send, part_recv,
):
    nb, ng, ny, nc, rows, chunks = sizes
    nz, nx = nb // ny, ng // nc
    count = nb * ng
    groups = nb * A_DEV // LANES
    per_group = LANES // A_DEV
    b, g = lax.axis_index("blk"), lax.axis_index("grp")
    z, y = b // ny, b % ny
    x, c = g // nc, g % nc
    me = b * ng + g

    load = pltpu.make_async_copy(emb_hbm, emb, emb_sem)
    load.start()

    barrier = pltpu.get_barrier_semaphore()

    def greet(step, carry):
        t = (me + step) % count
        pl.semaphore_signal(barrier, inc=1, device_id=(t // ng, t % ng), device_id_type=MESH)
        return carry

    lax.fori_loop(1, count, greet, 0)

    lab_row = lab_ref[...]
    lab_tile = jnp.broadcast_to(lab_row, (8, LANES))
    lab_k[g] = lab_tile
    lab_a[b] = lab_tile

    load.wait()
    values = emb[...].astype(jnp.float32)
    unit = (values * lax.rsqrt(jnp.sum(values * values, axis=1, keepdims=True) + 1e-06)).astype(jnp.bfloat16)

    def key_at(block, chunk=None):
        if chunk is None:
            return keys.at[pl.ds(pl.multiple_of(block * rows, rows), rows)]
        size = rows // chunks
        return keys.at[pl.ds(pl.multiple_of(block * rows + chunk * size, size), size)]

    def anc_at(block):
        return anc.at[pl.ds(pl.multiple_of(block * A_DEV, A_DEV), A_DEV)]

    key_at(g)[...] = unit
    anc_at(b)[...] = unit[:A_DEV]
    pl.semaphore_wait(barrier, count - 1)

    sends = []

    def send(src, dst, send_sem, recv_sem, device):
        copy = pltpu.make_async_remote_copy(
            src_ref=src, dst_ref=dst, send_sem=send_sem, recv_sem=recv_sem,
            device_id=device, device_id_type=MESH,
        )
        copy.start()
        sends.append(copy)

    def arrived(ref, sem):
        pltpu.make_async_copy(ref, ref, sem).wait()

    slot = 0
    for step in range(1, nz):
        to, _ = partner(z, step, nz)
        send(anc_at(b), anc_at(b), anc_send.at[slot], anc_recv.at[b], (to * ny + y, g))
        slot += 1
    kslot = 0
    for chunk in range(chunks):
        for step in range(1, nx):
            to, _ = partner(x, step, nx)
            send(key_at(g, chunk), key_at(g, chunk), key_send.at[kslot], key_recv.at[g, chunk], (b, to * nc + c))
            kslot += 1
    for step in range(1, ny):
        send(anc_at(b), anc_at(b), anc_send.at[slot], anc_recv.at[b], (z * ny + partner(y, step, ny)[0], g))
        slot += 1
    for step in range(1, nc):
        for chunk in range(chunks):
            send(key_at(g, chunk), key_at(g, chunk), key_send.at[kslot], key_recv.at[g, chunk],
                 (b, x * nc + partner(c, step, nc)[0]))
            kslot += 1
    lslot = 0
    for step in range(1, nb):
        send(lab_a.at[b], lab_a.at[b], lab_send.at[lslot], lab_a_recv, ((b + step) % nb, g))
        lslot += 1
    for step in range(1, ng):
        send(lab_k.at[g], lab_k.at[g], lab_send.at[lslot], lab_k_recv, (b, (g + step) % ng))
        lslot += 1

    key_jobs = [(step, chunk) for chunk in range(chunks) for step in range(1, nx)]
    anc_jobs = list(range(1, nz))
    for turn in range(max(len(key_jobs), len(anc_jobs))):
        if turn < len(anc_jobs):
            source = partner(z, anc_jobs[turn], nz)[1] * ny + y
            arrived(anc_at(source), anc_recv.at[source])
            for step in range(1, ny):
                send(anc_at(source), anc_at(source), anc_send.at[slot], anc_recv.at[source],
                     (z * ny + partner(y, step, ny)[0], g))
                slot += 1
        if turn < len(key_jobs):
            step, chunk = key_jobs[turn]
            source = partner(x, step, nx)[1] * nc + c
            arrived(key_at(source, chunk), key_recv.at[source, chunk])
            for hop in range(1, nc):
                send(key_at(source, chunk), key_at(source, chunk), key_send.at[kslot], key_recv.at[source, chunk],
                     (b, x * nc + partner(c, hop, nc)[0]))
                kslot += 1
    if nb > 1:
        arrived(lab_a.at[pl.ds(0, nb - 1)], lab_a_recv)
    if ng > 1:
        arrived(lab_k.at[pl.ds(0, ng - 1)], lab_k_recv)
    for hop in range(1, ny):
        for step in range(nz):
            source = (partner(z, step, nz)[1] if step else z) * ny + partner(y, hop, ny)[1]
            arrived(anc_at(source), anc_recv.at[source])
    for hop in range(1, nc):
        for step in range(nx):
            source = (partner(x, step, nx)[1] if step else x) * nc + partner(c, hop, nc)[1]
            for chunk in range(chunks):
                arrived(key_at(source, chunk), key_recv.at[source, chunk])

    lane = lax.broadcasted_iota(jnp.int32, (8, LANES), 1)
    lane_full = lax.broadcasted_iota(jnp.int32, (rows, LANES), 1)
    row_full = lax.broadcasted_iota(jnp.int32, (rows, LANES), 0)
    anchor_labels = []
    for h in range(groups):
        tile = lab_a[h * per_group]
        for q in range(1, per_group):
            tile = jnp.where(lane // A_DEV == q, pltpu.roll(lab_a[h * per_group + q], q * A_DEV, 1), tile)
        anchor_labels.append(tile[:1])

    def fold(block, carry):
        at = pl.ds(pl.multiple_of(block * rows, rows), rows)
        score = lax.dot_general(
            keys[at], anc[...], (((1,), (1,)), ((), ())), preferred_element_type=jnp.float32
        ) * 10.0
        key_labels = jnp.transpose(jnp.broadcast_to(lab_k[block][:1], (LANES, LANES)))
        key_ids = (b * ng + block) * rows + row_full
        out = []
        for h in range(groups):
            part_score = score[:, h * LANES:(h + 1) * LANES]
            anchor_block = h * per_group + lane_full // A_DEV
            anchor_ids = (anchor_block * ng + g) * rows + lane_full % A_DEV
            self_mask = anchor_ids == key_ids
            expo = jnp.where(self_mask, 0.0, jnp.exp(part_score - 10.0))
            positive = (key_labels == anchor_labels[h]) & jnp.logical_not(self_mask)
            out += [
                carry[3 * h] + jnp.sum(expo, axis=0, keepdims=True),
                carry[3 * h + 1] + jnp.sum(jnp.where(positive, part_score, 0.0), axis=0, keepdims=True),
                carry[3 * h + 2] + jnp.sum(jnp.where(positive, 1.0, 0.0), axis=0, keepdims=True),
            ]
        return tuple(out)

    zero = jnp.zeros((1, LANES), jnp.float32)
    totals = lax.fori_loop(0, ng, fold, (zero,) * (3 * groups), unroll=ng <= 4)
    tall = part.shape[1]
    pad = [jnp.zeros((tall - 3 * groups, LANES), jnp.float32)] if tall > 3 * groups else []
    part[me] = jnp.concatenate(list(totals) + pad, axis=0)

    def tell(step, carry):
        t = (me + step) % count
        pltpu.make_async_remote_copy(
            src_ref=part.at[me], dst_ref=part.at[me], send_sem=part_send, recv_sem=part_recv,
            device_id=(t // ng, t % ng), device_id_type=MESH,
        ).start()
        return carry

    lax.fori_loop(1, count, tell, 0)
    for copy in sends:
        copy.wait_send()
    arrived(part.at[pl.ds(0, count - 1)], part_recv)

    every = jnp.sum(part[...].reshape(nb, ng, tall, LANES), axis=0)
    loss_total, valid_total, own = zero, zero, zero
    for other in range(ng):
        for h in range(groups):
            denom = every[other, 3 * h:3 * h + 1]
            pos_sum = every[other, 3 * h + 1:3 * h + 2]
            number = every[other, 3 * h + 2:3 * h + 3]
            valid = number > 0.0
            loss = jnp.where(valid, jnp.log(denom) + 10.0 - pos_sum / jnp.maximum(number, 1.0), 0.0)
            loss_total += loss
            valid_total += jnp.where(valid, 1.0, 0.0)
            own = jnp.where(g * groups + b // per_group == other * groups + h, loss, own)
    total = jnp.sum(loss_total, axis=1, keepdims=True)
    valid_sum = jnp.sum(valid_total, axis=1, keepdims=True)
    mean = total / jnp.maximum(valid_sum, 1.0)
    shift = (LANES - (b % per_group) * A_DEV) % LANES
    own = pltpu.roll(jnp.broadcast_to(own, (8, LANES)), shift, 1)
    sub = lax.broadcasted_iota(jnp.int32, (8, LANES), 0)
    out_ref[...] = jnp.where(sub == 0, own, jnp.broadcast_to(mean, (8, LANES)))
    arrived(part.at[pl.ds(0, count - 1)], part_send)


def solution(mesh):
    nb, ng = mesh.shape["blk"], mesh.shape["grp"]
    ny = 2 if nb % 2 == 0 else 1
    nc = 2 if ng % 2 == 0 else 1

    def local(embeddings, labels):
        rows, width = embeddings.shape
        chunks = 4
        groups = nb * A_DEV // LANES
        tall = -(-3 * groups // 8) * 8
        sizes = (nb, ng, ny, nc, rows, chunks)
        dma = pltpu.SemaphoreType.DMA
        out = pl.pallas_call(
            functools.partial(kernel, sizes),
            name="contrast",
            out_shape=jax.ShapeDtypeStruct((8, LANES), jnp.float32),
            in_specs=[pl.BlockSpec(memory_space=pl.ANY), pl.BlockSpec(memory_space=pltpu.VMEM)],
            out_specs=pl.BlockSpec(memory_space=pltpu.VMEM),
            scratch_shapes=[
                pltpu.VMEM((rows, width), jnp.bfloat16),
                pltpu.VMEM((ng * rows, width), jnp.bfloat16),
                pltpu.VMEM((nb * A_DEV, width), jnp.bfloat16),
                pltpu.VMEM((ng, 8, LANES), jnp.int32),
                pltpu.VMEM((nb, 8, LANES), jnp.int32),
                pltpu.VMEM((nb * ng, tall, LANES), jnp.float32),
                dma,
                dma((ng * chunks,)),
                dma((ng, chunks)),
                dma((nb,)),
                dma((nb,)),
                dma((nb + ng,)),
                dma,
                dma,
                dma,
                dma,
            ],
            compiler_params=pltpu.CompilerParams(
                collective_id=0, has_side_effects=True, vmem_limit_bytes=48 * 1024 * 1024
            ),
        )(embeddings, labels.reshape(1, rows))
        return out[0, :A_DEV], out[1, 0]

    placed = (P(("blk", "grp"), None), P(("blk", "grp")))
    return jax.shard_map(
        local, mesh=mesh, in_specs=placed, out_specs=(P(("blk", "grp")), P()), check_vma=False
    )
```

```python
import functools

import jax
import jax.numpy as jnp
from jax import lax
from jax.experimental import pallas as pl
from jax.experimental.pallas import tpu as pltpu
from jax.sharding import PartitionSpec as P

A_DEV = 32
LANES = 128
MESH = pl.DeviceIdType.MESH


def flip(value, bits):
    out, bit = value, 1
    while bit <= bits:
        if bits & bit:
            out = out + bit - 2 * bit * ((value // bit) % 2)
        bit *= 2
    return out


def partner(value, step, count):
    if count & (count - 1) == 0:
        other = flip(value, step)
        return other, other
    return (value + step) % count, (value + count - step) % count


def kernel(
    sizes, emb_hbm, lab_hbm, out_ref,
    emb, lab_ref, keys, anc, lab_k, lab_a, lab_col, part,
    emb_sem, lab_sem, key_send, key_recv, anc_send, anc_recv, lab_send, lab_k_recv, lab_a_recv, part_send, part_recv,
):
    nb, ng, ny, nc, rows, chunks, cuts = sizes
    nz, nx = nb // ny, ng // nc
    count = nb * ng
    groups = nb * A_DEV // LANES
    per_group = LANES // A_DEV
    b, g = lax.axis_index("blk"), lax.axis_index("grp")
    z, y = b // ny, b % ny
    x, c = g // nc, g % nc
    me = b * ng + g

    load = pltpu.make_async_copy(emb_hbm, emb, emb_sem)
    load.start()
    load_labels = pltpu.make_async_copy(lab_hbm, lab_ref, lab_sem)
    load_labels.start()

    barrier = pltpu.get_barrier_semaphore()

    for step in range(1, nb):
        pl.semaphore_signal(barrier, inc=1, device_id=((b + step) % nb, g), device_id_type=MESH)
    for step in range(1, ng):
        pl.semaphore_signal(barrier, inc=1, device_id=(b, (g + step) % ng), device_id_type=MESH)

    load_labels.wait()
    lab_row = lab_ref[...]
    lab_k[g] = lab_row
    lab_a[b] = lab_row

    load.wait()
    values = emb[...].astype(jnp.float32)
    unit = (values * lax.rsqrt(jnp.sum(values * values, axis=1, keepdims=True) + 1e-06)).astype(jnp.bfloat16)

    def key_at(block, chunk=None):
        if chunk is None:
            return keys.at[pl.ds(pl.multiple_of(block * rows, rows), rows)]
        size = rows // chunks
        return keys.at[pl.ds(pl.multiple_of(block * rows + chunk * size, size), size)]

    piece = A_DEV // cuts

    def anc_at(block, cut=None):
        if cut is None:
            return anc.at[pl.ds(pl.multiple_of(block * A_DEV, A_DEV), A_DEV)]
        return anc.at[pl.ds(pl.multiple_of(block * A_DEV + cut * piece, piece), piece)]

    key_at(g)[...] = unit
    anc_at(b)[...] = unit[:A_DEV]
    pl.semaphore_wait(barrier, nb + ng - 2)

    sends = []

    def send(src, dst, send_sem, recv_sem, device):
        copy = pltpu.make_async_remote_copy(
            src_ref=src, dst_ref=dst, send_sem=send_sem, recv_sem=recv_sem,
            device_id=device, device_id_type=MESH,
        )
        copy.start()
        sends.append(copy)

    def arrived(ref, sem):
        pltpu.make_async_copy(ref, ref, sem).wait()

    lslot = 0
    for step in range(1, nb):
        send(lab_a.at[b], lab_a.at[b], lab_send.at[lslot], lab_a_recv, ((b + step) % nb, g))
        lslot += 1
    for step in range(1, ng):
        send(lab_k.at[g], lab_k.at[g], lab_send.at[lslot], lab_k_recv, (b, (g + step) % ng))
        lslot += 1
    slot, kslot = 0, 0

    def send_anchors(block, cut, device):
        nonlocal slot
        send(anc_at(block, cut), anc_at(block, cut), anc_send.at[slot], anc_recv.at[block, cut], device)
        slot += 1

    def send_keys(block, chunk, device):
        nonlocal kslot
        send(key_at(block, chunk), key_at(block, chunk), key_send.at[kslot], key_recv.at[block, chunk], device)
        kslot += 1

    for chunk in range(chunks):
        for step in range(1, nx):
            send_keys(g, chunk, (b, partner(x, step, nx)[0] * nc + c))
    for step in range(1, nz):
        for cut in range(cuts):
            send_anchors(b, cut, (partner(z, step, nz)[0] * ny + y, g))
    for cut in range(cuts):
        for step in range(1, ny):
            send_anchors(b, cut, (z * ny + partner(y, step, ny)[0], g))
    for step in range(1, nc):
        for chunk in range(chunks):
            send_keys(g, chunk, (b, x * nc + partner(c, step, nc)[0]))

    key_jobs = [(step, chunk) for chunk in range(chunks) for step in range(1, nx)]
    anc_jobs = [(step, cut) for step in range(1, nz) for cut in range(cuts)]
    jobs = [((at + 1) / len(key_jobs), 0, job) for at, job in enumerate(key_jobs)]
    jobs += [((at + 1) / len(anc_jobs), 1, job) for at, job in enumerate(anc_jobs)]
    for _, kind, (step, number) in sorted(jobs):
        if kind:
            source = partner(z, step, nz)[1] * ny + y
            arrived(anc_at(source, number), anc_recv.at[source, number])
            for hop in range(1, ny):
                send_anchors(source, number, (z * ny + partner(y, hop, ny)[0], g))
        else:
            source = partner(x, step, nx)[1] * nc + c
            arrived(key_at(source, number), key_recv.at[source, number])
            for hop in range(1, nc):
                send_keys(source, number, (b, x * nc + partner(c, hop, nc)[0]))

    if nb > 1:
        arrived(lab_a.at[pl.ds(0, nb - 1)], lab_a_recv)
    if ng > 1:
        arrived(lab_k.at[pl.ds(0, ng - 1)], lab_k_recv)
    for block in range(ng):
        lab_col[block] = jnp.transpose(jnp.broadcast_to(lab_k[block], (LANES, LANES)))

    lane = lax.broadcasted_iota(jnp.int32, (8, LANES), 1)
    lane_full = lax.broadcasted_iota(jnp.int32, (rows, LANES), 1)
    row_full = lax.broadcasted_iota(jnp.int32, (rows, LANES), 0)

    for hop in range(1, nc):
        for step in range(nx):
            source = (partner(x, step, nx)[1] if step else x) * nc + partner(c, hop, nc)[1]
            for chunk in range(chunks):
                arrived(key_at(source, chunk), key_recv.at[source, chunk])

    zero = jnp.zeros((1, LANES), jnp.float32)

    def fold_group(h):
        tile = jnp.broadcast_to(lab_a[h * per_group], (8, LANES))
        for q in range(1, per_group):
            turned = pltpu.roll(jnp.broadcast_to(lab_a[h * per_group + q], (8, LANES)), q * A_DEV, 1)
            tile = jnp.where(lane // A_DEV == q, turned, tile)
        labels_here = tile[:1]
        anchors = anc[pl.ds(pl.multiple_of(h * LANES, LANES), LANES)]
        anchor_ids = ((h * per_group + lane_full // A_DEV) * ng + g) * rows + lane_full % A_DEV

        def fold(block, carry):
            at = pl.ds(pl.multiple_of(block * rows, rows), rows)
            score = lax.dot_general(
                keys[at], anchors, (((1,), (1,)), ((), ())), preferred_element_type=jnp.float32
            ) * 10.0
            self_mask = anchor_ids == (b * ng + block) * rows + row_full
            expo = jnp.where(self_mask, 0.0, jnp.exp(score - 10.0))
            positive = (lab_col[block] == labels_here) & jnp.logical_not(self_mask)
            return (
                carry[0] + jnp.sum(expo, axis=0, keepdims=True),
                carry[1] + jnp.sum(jnp.where(positive, score, 0.0), axis=0, keepdims=True),
                carry[2] + jnp.sum(jnp.where(positive, 1.0, 0.0), axis=0, keepdims=True),
            )

        return jnp.concatenate(lax.fori_loop(0, ng, fold, (zero,) * 3, unroll=ng <= 4), axis=0)

    near, per_z = b // per_group, max(per_group // ny, 1)
    in_step = nz & (nz - 1) == 0 and groups & (groups - 1) == 0 and per_group % ny == 0
    found = []
    for turn in range(groups):
        first = turn * per_z if in_step else (0 if turn == 0 else nz)
        last = first + per_z if in_step else nz
        for step in range(first, last):
            for hop in range(1, ny):
                source = (partner(z, step, nz)[1] if step else z) * ny + partner(y, hop, ny)[1]
                for cut in range(cuts):
                    arrived(anc_at(source, cut), anc_recv.at[source, cut])
        h = partner(near, turn, groups)[0] if turn else near
        found.append((h, fold_group(h)))
    for h in range(groups):
        mine = found[0][1]
        for other, sums in found[1:]:
            mine = jnp.where(other == h, sums, mine)
        part[me, 3 * h:3 * h + 3] = mine

    def tell(step, carry):
        t = (me + step) % count
        pltpu.make_async_remote_copy(
            src_ref=part.at[me], dst_ref=part.at[me], send_sem=part_send, recv_sem=part_recv,
            device_id=(t // ng, t % ng), device_id_type=MESH,
        ).start()
        return carry

    lax.fori_loop(1, count, tell, 0, unroll=count <= 32)
    for copy in sends:
        copy.wait_send()
    arrived(part.at[pl.ds(0, count - 1)], part_recv)

    tall = part.shape[1]
    every = jnp.sum(part[...].reshape(nb, ng, tall, LANES), axis=0)
    loss_total, valid_total, own = zero, zero, zero
    for other in range(ng):
        for h in range(groups):
            denom = every[other, 3 * h:3 * h + 1]
            pos_sum = every[other, 3 * h + 1:3 * h + 2]
            number = every[other, 3 * h + 2:3 * h + 3]
            valid = number > 0.0
            loss = jnp.where(valid, jnp.log(denom) + 10.0 - pos_sum / jnp.maximum(number, 1.0), 0.0)
            loss_total += loss
            valid_total += jnp.where(valid, 1.0, 0.0)
            own = jnp.where(g * groups + b // per_group == other * groups + h, loss, own)
    total = jnp.sum(loss_total, axis=1, keepdims=True)
    valid_sum = jnp.sum(valid_total, axis=1, keepdims=True)
    mean = total / jnp.maximum(valid_sum, 1.0)
    shift = (LANES - (b % per_group) * A_DEV) % LANES
    own = pltpu.roll(jnp.broadcast_to(own, (8, LANES)), shift, 1)
    sub = lax.broadcasted_iota(jnp.int32, (8, LANES), 0)
    out_ref[...] = jnp.where(sub == 0, own, jnp.broadcast_to(mean, (8, LANES)))
    arrived(part.at[pl.ds(0, count - 1)], part_send)


def solution(mesh):
    nb, ng = mesh.shape["blk"], mesh.shape["grp"]
    ny = 2 if nb % 2 == 0 else 1
    nc = 2 if ng % 2 == 0 else 1

    def local(embeddings, labels):
        rows, width = embeddings.shape
        chunks, cuts = 4, 2
        groups = nb * A_DEV // LANES
        tall = 3 * groups
        sizes = (nb, ng, ny, nc, rows, chunks, cuts)
        dma = pltpu.SemaphoreType.DMA
        out = pl.pallas_call(
            functools.partial(kernel, sizes),
            name="contrast",
            out_shape=jax.ShapeDtypeStruct((8, LANES), jnp.float32),
            in_specs=[pl.BlockSpec(memory_space=pl.ANY)] * 2,
            out_specs=pl.BlockSpec(memory_space=pltpu.VMEM),
            scratch_shapes=[
                pltpu.VMEM((rows, width), jnp.bfloat16),
                pltpu.VMEM((1, rows), jnp.int32),
                pltpu.VMEM((ng * rows, width), jnp.bfloat16),
                pltpu.VMEM((nb * A_DEV, width), jnp.bfloat16),
                pltpu.VMEM((ng, 1, LANES), jnp.int32),
                pltpu.VMEM((nb, 1, LANES), jnp.int32),
                pltpu.VMEM((ng, rows, LANES), jnp.int32),
                pltpu.VMEM((nb * ng, tall, LANES), jnp.float32),
                dma,
                dma,
                dma((ng * chunks,)),
                dma((ng, chunks)),
                dma((nb * cuts,)),
                dma((nb, cuts)),
                dma((nb + ng,)),
                dma,
                dma,
                dma,
                dma,
            ],
            compiler_params=pltpu.CompilerParams(
                collective_id=0, has_side_effects=True
            ),
        )(embeddings, labels.reshape(1, rows))
        return out[0, :A_DEV], out[1, 0]

    placed = (P(("blk", "grp"), None), P(("blk", "grp")))
    return jax.shard_map(
        local, mesh=mesh, in_specs=placed, out_specs=(P(("blk", "grp")), P()), check_vma=False
    )
```

```python
import functools

import jax
import jax.numpy as jnp
from jax import lax
from jax.experimental import pallas as pl
from jax.experimental.pallas import tpu as pltpu
from jax.sharding import PartitionSpec as P

A_DEV = 32
LANES = 128
MESH = pl.DeviceIdType.MESH


def flip(value, bits):
    out, bit = value, 1
    while bit <= bits:
        if bits & bit:
            out = out + bit - 2 * bit * ((value // bit) % 2)
        bit *= 2
    return out


def partner(value, step, count):
    if count & (count - 1) == 0:
        other = flip(value, step)
        return other, other
    return (value + step) % count, (value + count - step) % count


def kernel(
    sizes, emb_hbm, lab_hbm, out_ref,
    emb, lab_ref, keys, anc, lab_k, lab_a, lab_col, part,
    emb_sem, lab_sem, key_send, key_recv, anc_send, anc_recv, lab_send, lab_k_recv, lab_a_recv, part_send, part_recv,
):
    nb, ng, ny, nc, rows, chunks, cuts = sizes
    nz, nx = nb // ny, ng // nc
    count = nb * ng
    groups = nb * A_DEV // LANES
    per_group = LANES // A_DEV
    b, g = lax.axis_index("blk"), lax.axis_index("grp")
    z, y = b // ny, b % ny
    x, c = g // nc, g % nc
    me = b * ng + g

    load = pltpu.make_async_copy(emb_hbm, emb, emb_sem)
    load.start()
    load_labels = pltpu.make_async_copy(lab_hbm, lab_ref, lab_sem)
    load_labels.start()

    barrier = pltpu.get_barrier_semaphore()

    for step in range(1, nb):
        pl.semaphore_signal(barrier, inc=1, device_id=((b + step) % nb, g), device_id_type=MESH)
    for step in range(1, ng):
        pl.semaphore_signal(barrier, inc=1, device_id=(b, (g + step) % ng), device_id_type=MESH)

    load_labels.wait()
    lab_row = lab_ref[...]
    lab_k[g] = lab_row
    lab_a[b] = lab_row

    load.wait()
    values = emb[...].astype(jnp.float32)
    unit = (values * lax.rsqrt(jnp.sum(values * values, axis=1, keepdims=True) + 1e-06)).astype(jnp.bfloat16)

    def key_at(block, chunk=None):
        if chunk is None:
            return keys.at[pl.ds(pl.multiple_of(block * rows, rows), rows)]
        size = rows // chunks
        return keys.at[pl.ds(pl.multiple_of(block * rows + chunk * size, size), size)]

    piece = A_DEV // cuts

    def anc_at(block, cut=None):
        if cut is None:
            return anc.at[pl.ds(pl.multiple_of(block * A_DEV, A_DEV), A_DEV)]
        return anc.at[pl.ds(pl.multiple_of(block * A_DEV + cut * piece, piece), piece)]

    key_at(g)[...] = unit
    anc_at(b)[...] = unit[:A_DEV]
    pl.semaphore_wait(barrier, nb + ng - 2)

    sends = []

    def send(src, dst, send_sem, recv_sem, device):
        copy = pltpu.make_async_remote_copy(
            src_ref=src, dst_ref=dst, send_sem=send_sem, recv_sem=recv_sem,
            device_id=device, device_id_type=MESH,
        )
        copy.start()
        sends.append(copy)

    def arrived(ref, sem):
        pltpu.make_async_copy(ref, ref, sem).wait()

    lslot = 0
    for step in range(1, nb):
        send(lab_a.at[b], lab_a.at[b], lab_send.at[lslot], lab_a_recv, ((b + step) % nb, g))
        lslot += 1
    for step in range(1, ng):
        send(lab_k.at[g], lab_k.at[g], lab_send.at[lslot], lab_k_recv, (b, (g + step) % ng))
        lslot += 1
    slot, kslot = 0, 0

    def send_anchors(block, cut, device):
        nonlocal slot
        send(anc_at(block, cut), anc_at(block, cut), anc_send.at[slot], anc_recv.at[block, cut], device)
        slot += 1

    def send_keys(block, chunk, device):
        nonlocal kslot
        send(key_at(block, chunk), key_at(block, chunk), key_send.at[kslot], key_recv.at[block, chunk], device)
        kslot += 1

    for chunk in range(chunks):
        for step in range(1, nx):
            send_keys(g, chunk, (b, partner(x, step, nx)[0] * nc + c))
    for step in range(1, nz):
        for cut in range(cuts):
            send_anchors(b, cut, (partner(z, step, nz)[0] * ny + y, g))
    for cut in range(cuts):
        for step in range(1, ny):
            send_anchors(b, cut, (z * ny + partner(y, step, ny)[0], g))
    for step in range(1, nc):
        for chunk in range(chunks):
            send_keys(g, chunk, (b, x * nc + partner(c, step, nc)[0]))

    key_jobs = [(step, chunk) for chunk in range(chunks) for step in range(1, nx)]
    anc_jobs = [(step, cut) for step in range(1, nz) for cut in range(cuts)]
    jobs = [((at + 1) / len(key_jobs), 0, job) for at, job in enumerate(key_jobs)]
    jobs += [((at + 1) / len(anc_jobs), 1, job) for at, job in enumerate(anc_jobs)]
    for _, kind, (step, number) in sorted(jobs):
        if kind:
            source = partner(z, step, nz)[1] * ny + y
            arrived(anc_at(source, number), anc_recv.at[source, number])
            for hop in range(1, ny):
                send_anchors(source, number, (z * ny + partner(y, hop, ny)[0], g))
        else:
            source = partner(x, step, nx)[1] * nc + c
            arrived(key_at(source, number), key_recv.at[source, number])
            for hop in range(1, nc):
                send_keys(source, number, (b, x * nc + partner(c, hop, nc)[0]))

    if nb > 1:
        arrived(lab_a.at[pl.ds(0, nb - 1)], lab_a_recv)
    if ng > 1:
        arrived(lab_k.at[pl.ds(0, ng - 1)], lab_k_recv)
    for block in range(ng):
        lab_col[block] = jnp.transpose(jnp.broadcast_to(lab_k[block], (LANES, LANES)))

    lane = lax.broadcasted_iota(jnp.int32, (8, LANES), 1)
    lane_full = lax.broadcasted_iota(jnp.int32, (rows, LANES), 1)
    row_full = lax.broadcasted_iota(jnp.int32, (rows, LANES), 0)

    for hop in range(1, nc):
        for step in range(nx):
            source = (partner(x, step, nx)[1] if step else x) * nc + partner(c, hop, nc)[1]
            for chunk in range(chunks):
                arrived(key_at(source, chunk), key_recv.at[source, chunk])

    zero = jnp.zeros((1, LANES), jnp.float32)

    def fold_group(h):
        tile = jnp.broadcast_to(lab_a[h * per_group], (8, LANES))
        for q in range(1, per_group):
            turned = pltpu.roll(jnp.broadcast_to(lab_a[h * per_group + q], (8, LANES)), q * A_DEV, 1)
            tile = jnp.where(lane // A_DEV == q, turned, tile)
        labels_here = tile[:1]
        anchors = anc[pl.ds(pl.multiple_of(h * LANES, LANES), LANES)]
        anchor_ids = ((h * per_group + lane_full // A_DEV) * ng + g) * rows + lane_full % A_DEV

        def fold(block, carry):
            at = pl.ds(pl.multiple_of(block * rows, rows), rows)
            score = lax.dot_general(
                keys[at], anchors, (((1,), (1,)), ((), ())), preferred_element_type=jnp.float32
            ) * 10.0
            self_mask = anchor_ids == (b * ng + block) * rows + row_full
            expo = jnp.where(self_mask, 0.0, jnp.exp(score - 10.0))
            positive = (lab_col[block] == labels_here) & jnp.logical_not(self_mask)
            return (
                carry[0] + jnp.sum(expo, axis=0, keepdims=True),
                carry[1] + jnp.sum(jnp.where(positive, score, 0.0), axis=0, keepdims=True),
                carry[2] + jnp.sum(jnp.where(positive, 1.0, 0.0), axis=0, keepdims=True),
            )

        return jnp.concatenate(lax.fori_loop(0, ng, fold, (zero,) * 3, unroll=ng <= 4), axis=0)

    near, per_z = b // per_group, max(per_group // ny, 1)
    in_step = nz & (nz - 1) == 0 and groups & (groups - 1) == 0 and per_group % ny == 0
    found = []
    for turn in range(groups):
        first = turn * per_z if in_step else (0 if turn == 0 else nz)
        last = first + per_z if in_step else nz
        for step in range(first, last):
            for hop in range(1, ny):
                source = (partner(z, step, nz)[1] if step else z) * ny + partner(y, hop, ny)[1]
                for cut in range(cuts):
                    arrived(anc_at(source, cut), anc_recv.at[source, cut])
        h = partner(near, turn, groups)[0] if turn else near
        found.append((h, fold_group(h)))
    for h in range(groups):
        mine = found[0][1]
        for other, sums in found[1:]:
            mine = jnp.where(other == h, sums, mine)
        part[me, 3 * h:3 * h + 3] = mine

    def tell(step, carry):
        t = (me + step) % count
        pltpu.make_async_remote_copy(
            src_ref=part.at[me], dst_ref=part.at[me], send_sem=part_send, recv_sem=part_recv,
            device_id=(t // ng, t % ng), device_id_type=MESH,
        ).start()
        return carry

    lax.fori_loop(1, count, tell, 0, unroll=count <= 32)
    for copy in sends:
        copy.wait_send()
    arrived(part.at[pl.ds(0, count - 1)], part_recv)

    tall = part.shape[1]
    every = jnp.sum(part[...].reshape(nb, ng, tall, LANES), axis=0)
    loss_total, valid_total, own = zero, zero, zero
    for other in range(ng):
        for h in range(groups):
            denom = every[other, 3 * h:3 * h + 1]
            pos_sum = every[other, 3 * h + 1:3 * h + 2]
            number = every[other, 3 * h + 2:3 * h + 3]
            valid = number > 0.0
            loss = jnp.where(valid, jnp.log(denom) + 10.0 - pos_sum / jnp.maximum(number, 1.0), 0.0)
            loss_total += loss
            valid_total += jnp.where(valid, 1.0, 0.0)
            own = jnp.where(g * groups + b // per_group == other * groups + h, loss, own)
    total = jnp.sum(loss_total, axis=1, keepdims=True)
    valid_sum = jnp.sum(valid_total, axis=1, keepdims=True)
    mean = total / jnp.maximum(valid_sum, 1.0)
    shift = (LANES - (b % per_group) * A_DEV) % LANES
    own = pltpu.roll(jnp.broadcast_to(own, (8, LANES)), shift, 1)
    sub = lax.broadcasted_iota(jnp.int32, (8, LANES), 0)
    out_ref[...] = jnp.where(sub == 0, own, jnp.broadcast_to(mean, (8, LANES)))
    arrived(part.at[pl.ds(0, count - 1)], part_send)


def solution(mesh):
    nb, ng = mesh.shape["blk"], mesh.shape["grp"]
    ny = 2 if nb % 2 == 0 else 1
    nc = 2 if ng % 2 == 0 else 1

    def local(embeddings, labels):
        rows, width = embeddings.shape
        chunks, cuts = 4, 2
        groups = nb * A_DEV // LANES
        tall = 3 * groups
        sizes = (nb, ng, ny, nc, rows, chunks, cuts)
        dma = pltpu.SemaphoreType.DMA
        out = pl.pallas_call(
            functools.partial(kernel, sizes),
            name="contrast",
            out_shape=jax.ShapeDtypeStruct((8, LANES), jnp.float32),
            in_specs=[pl.BlockSpec(memory_space=pltpu.HBM)] * 2,
            out_specs=pl.BlockSpec(memory_space=pltpu.VMEM),
            scratch_shapes=[
                pltpu.VMEM((rows, width), jnp.bfloat16),
                pltpu.VMEM((1, rows), jnp.int32),
                pltpu.VMEM((ng * rows, width), jnp.bfloat16),
                pltpu.VMEM((nb * A_DEV, width), jnp.bfloat16),
                pltpu.VMEM((ng, 1, LANES), jnp.int32),
                pltpu.VMEM((nb, 1, LANES), jnp.int32),
                pltpu.VMEM((ng, rows, LANES), jnp.int32),
                pltpu.VMEM((nb * ng, tall, LANES), jnp.float32),
                dma,
                dma,
                dma((ng * chunks,)),
                dma((ng, chunks)),
                dma((nb * cuts,)),
                dma((nb, cuts)),
                dma((nb + ng,)),
                dma,
                dma,
                dma,
                dma,
            ],
            compiler_params=pltpu.CompilerParams(
                collective_id=0, has_side_effects=True, vmem_limit_bytes=48 * 1024 * 1024
            ),
        )(pltpu.with_memory_space_constraint(embeddings, pltpu.HBM), pltpu.with_memory_space_constraint(labels.reshape(1, rows), pltpu.HBM))
        return out[0, :A_DEV], out[1, 0]

    placed = (P(("blk", "grp"), None), P(("blk", "grp")))
    return jax.shard_map(
        local, mesh=mesh, in_specs=placed, out_specs=(P(("blk", "grp")), P()), check_vma=False
    )
```
